32 devices in a mesh: expert: 4 (over z), shard: 8 (over y, x, core).
Axes of the slice: x: 2, y: 2, z: 4, core: 2. Of those that a mesh axis runs over, the one named last changes fastest.
Arguments:
- master_gate: float32 [64, 2048, 1408], P('expert', 'shard'), may hold values from -0.1875 to 0.1875
- master_up: float32 [64, 2048, 1408], P('expert', 'shard'), may hold values from -0.1875 to 0.1875
- router_weight: float32 [2048, 64], P('shard', 'expert'), may hold values from -0.125 to 0.125
- router_gain: float32 [2048], P('shard'), may hold values from 0.25 to 1.75
Outputs:
- final_gate: bfloat16 [64, 2048, 1408], P('expert', None, 'shard')
- final_up: bfloat16 [64, 2048, 1408], P('expert', None, 'shard')
- scale_gate: float32 [64, 1408], P('expert', 'shard')
- scale_up: float32 [64, 1408], P('expert', 'shard')
- serve_router: bfloat16 [2048, 64], replicated
The draws below stay inside these ranges and needn't reach their ends.
All inputs are finite; a program needn't handle non-finite values.
Results may differ from the reference program's by a relative error of at most 0.001.
Values may be sent and summed in bfloat16 or wider, within the bound.
A program may use at most 192 MiB of HBM per device.

```python
import jax
import jax.numpy as jnp
from jax import lax

EXPERTS = 64
D_MODEL = 2048
D_EXPERT = 1408


def strengthened(entries, stream_key, source, target, blocks, factor):
    def block_of(position):
        return (jnp.arange(entries.shape[position]) // (entries.shape[position] // blocks)).reshape((-1,) + (1,) * (entries.ndim - 1 - position))

    one_side = jax.random.permutation(stream_key, blocks)[block_of(target)]
    second = (block_of(target) + blocks // 2) % blocks
    return jnp.where((block_of(source) == one_side) | (block_of(source) == second), factor * entries, entries)


def block_levels(key, dims, pieces, least, top_value):
    def one(position, shards_of):
        heights = jax.random.uniform(jax.random.fold_in(jax.random.fold_in(key, 6), position), (shards_of,), jnp.float32, least / len(pieces), top_value / len(pieces))
        return jnp.repeat(jnp.exp(heights), dims[position] // shards_of).reshape((-1,) + (1,) * (len(dims) - position - 1))

    level = one(*pieces[0])
    for cut in pieces[1:]:
        level = level * one(*cut)
    return level


def bell_draw(own_key, extent, deviation, limit, pieces=(), held_as=jnp.bfloat16):
    result = deviation * jax.random.normal(own_key, extent, jnp.float32)
    if pieces:
        result = result * block_levels(own_key, extent, pieces, -0.22, 0.18)
    return jnp.clip(result, -limit, limit).astype(held_as)


def gaussian_with(rng, shape, width, bound, pieces, heavy, kind=jnp.bfloat16):
    entries = width * jax.random.normal(rng, shape, jnp.float32)
    if pieces:
        entries = entries * block_levels(rng, shape, pieces, -0.22, 0.18)
    return jnp.clip(strengthened(entries, jax.random.fold_in(rng, 3), *heavy), -bound, bound).astype(kind)


def setup_inputs(seed: int = 0) -> dict:
    seeds = jax.random.split(jax.random.key(seed), 5)
    master_gate = gaussian_with(seeds[0], (EXPERTS, D_MODEL, D_EXPERT), D_MODEL ** -0.5, 0.1875, ((0, 4), (1, 8)), (1, 2, 8, 2.0), jnp.float32)
    master_up = gaussian_with(seeds[1], (EXPERTS, D_MODEL, D_EXPERT), D_MODEL ** -0.5, 0.1875, ((0, 4), (1, 8)), (1, 2, 8, 2.0), jnp.float32)
    router_weight = bell_draw(seeds[2], (D_MODEL, EXPERTS), D_MODEL ** -0.5, 0.125, ((0, 8), (1, 4)), jnp.float32)
    router_gain = jnp.clip(1.0 + 0.15 * jax.random.normal(seeds[3], (D_MODEL,), jnp.float32), 0.25, 1.75)
    return dict(master_gate=master_gate, master_up=master_up, router_weight=router_weight, router_gain=router_gain)


def reference(master_gate, master_up, router_weight, router_gain):
    scale_gate = jnp.sqrt(lax.optimization_barrier(jnp.sum(master_gate * master_gate, axis=1)))
    final_gate = (master_gate / jnp.expand_dims(scale_gate, 1)).astype(jnp.bfloat16)
    scale_up = jnp.sqrt(lax.optimization_barrier(jnp.sum(master_up * master_up, axis=1)))
    final_up = (master_up / jnp.expand_dims(scale_up, 1)).astype(jnp.bfloat16)
    serve_router = (router_weight * router_gain[:, None]).astype(jnp.bfloat16)
    return (final_gate, final_up, scale_gate, scale_up, serve_router)
```

```python
import functools

import jax
import jax.numpy as jnp
from jax import lax
from jax.experimental import pallas as pl
from jax.experimental.pallas import tpu as pltpu
from jax.sharding import PartitionSpec as P

LANES = 128
FIRST = 3
RING = 6
STREAM = 6
SLOTS = 4
DEPTH = 2
VMEM_LIMIT = 67043328
SPARE = 4194304

def plain(master_gate, master_up, router_weight, router_gain):
    total_gate, total_up = lax.psum(
        (jnp.sum(master_gate * master_gate, axis=1), jnp.sum(master_up * master_up, axis=1)),
        "shard",
    )
    scale_gate = jnp.sqrt(total_gate)
    scale_up = jnp.sqrt(total_up)
    narrow_gate, narrow_up = (
        (master_gate / jnp.expand_dims(scale_gate, 1)).astype(jnp.bfloat16),
        (master_up / jnp.expand_dims(scale_up, 1)).astype(jnp.bfloat16),
    )
    final_gate, final_up = (
        lax.all_to_all(narrow_gate, "shard", split_axis=2, concat_axis=1, tiled=True),
        lax.all_to_all(narrow_up, "shard", split_axis=2, concat_axis=1, tiled=True),
    )
    scale_gate = lax.dynamic_slice_in_dim(
        scale_gate, lax.axis_index("shard") * final_gate.shape[2], final_gate.shape[2], axis=1
    )
    scale_up = lax.dynamic_slice_in_dim(
        scale_up, lax.axis_index("shard") * final_up.shape[2], final_up.shape[2], axis=1
    )
    part_router = (router_weight * router_gain[:, None]).astype(jnp.bfloat16)
    row_router = lax.all_gather(part_router, "shard", axis=0, tiled=True)
    serve_router = lax.all_gather(row_router, "expert", axis=1, tiled=True)
    return (final_gate, final_up, scale_gate, scale_up, serve_router)


def partner(me, n, mask):
    index, bit = 0, 1
    while bit < n:
        mine = lax.rem(me // bit, 2)
        index = index + bit * (1 - mine if mask & bit else mine)
        bit *= 2
    return index


def phases_of(n):
    if n == 8:
        return ((6, 1), (2, 4), (7,), (3, 5))
    return tuple((mask,) for mask in range(1, n))


def stages_of(n):
    doubling = []
    bit = 2
    while bit < n:
        doubling.append((bit,))
        bit *= 2
    return ((tuple(range(2, n, 2)),), tuple(doubling))


def peers_of(stages):
    return sum(len(stage) for stage in stages)


def remote(source, target, send, recv, device):
    return pltpu.make_async_remote_copy(
        src_ref=source, dst_ref=target, send_sem=send, recv_sem=recv,
        device_id=device, device_id_type=pl.DeviceIdType.MESH)


def kernel(n, nz, gate, up, weight, gain, out, scale_gate, scale_up, router_out,
           buf, stream, slots, part0, got0, run0, total0, part1, got1, run1, total1,
           scales, inverse, weight_in, gain_in, piece, column,
           load_sem, stream_sem, router_sem, send_sem, recv_sem, raw_sem,
           send0, recv0, send1, recv1, first_send, first_recv, second_send, second_recv):
    me = lax.axis_index("shard")
    mez = lax.axis_index("expert")
    core = lax.rem(me, 2)
    experts, rows, width = gate.shape
    slabs = 2 * experts
    narrow = width // n
    tiles = width // LANES
    router_rows = weight.shape[0]
    phases = phases_of(n)
    sources = (gate, up)

    def load(src, e):
        k = 2 * e + src
        return pltpu.make_async_copy(sources[src].at[e], buf.at[k % RING], load_sem.at[k % RING])

    def flow(src, e):
        k = (2 * (e - FIRST) + src) % STREAM
        return pltpu.make_async_copy(sources[src].at[e], stream.at[k], stream_sem.at[k])

    for e in range(FIRST):
        for src in range(2):
            load(src, e).start()
    weight_load = pltpu.make_async_copy(weight, weight_in, router_sem.at[0])
    gain_load = pltpu.make_async_copy(gain, gain_in, router_sem.at[1])
    weight_load.start()
    gain_load.start()
    for e in range(FIRST, FIRST + STREAM // 2):
        for src in range(2):
            flow(src, e).start()

    barrier = pltpu.get_barrier_semaphore()
    for mask in range(1, n):
        pl.semaphore_signal(barrier, inc=1, device_id={"shard": partner(me, n, mask)},
                            device_id_type=pl.DeviceIdType.MESH)
    for r in range(1, nz):
        pl.semaphore_signal(barrier, inc=1, device_id={"expert": lax.rem(mez + r, nz)},
                            device_id_type=pl.DeviceIdType.MESH)

    my_lanes = pl.ds(pl.multiple_of(me * rows, rows), rows)
    my_rows = pl.ds(pl.multiple_of(me * narrow, 16), narrow)

    def slab_copy(src, e, mask, raw=False):
        s = (2 * e + src) % SLOTS
        target = partner(me, n, mask)
        return remote(
            slots.at[s, pl.ds(pl.multiple_of(target * narrow, 16), narrow), :],
            out.at[src * experts + e, :, my_lanes],
            send_sem.at[s, mask - 1],
            (raw_sem if raw else recv_sem).at[src, mask - 1],
            {"shard": target})

    def wait_phase(src, e, q, raw=False):
        for mask in phases[q]:
            slab_copy(src, e, mask, raw).wait_send()

    def phase(src, e, q):
        back = q - DEPTH
        before = src
        while back < 0:
            back += len(phases)
            before -= 1
        lag_e = e + before // 2
        if not isinstance(lag_e, int) or lag_e >= 0:
            wait_phase(before % 2, lag_e, back)
        raw = isinstance(e, int) and e == 0
        for mask in phases[q]:
            slab_copy(src, e, mask, raw).start()

    def narrow_slab(src, e, raw=False):
        k = 2 * e + src
        b, s = k % RING, k % SLOTS
        if not isinstance(e, int) or e >= FIRST:
            load(src, e).wait()

        def tile(j, _):
            lanes = pl.ds(pl.multiple_of(j * LANES, LANES), LANES)
            y = buf[b, :, lanes]
            if not raw:
                y = y * inverse[src, j, pl.ds(e, 1), :]
            slots[s, lanes, :] = y.T.astype(jnp.bfloat16)
            return 0

        lax.fori_loop(0, tiles, tile, 0)
        out[src * experts + e, :, my_lanes] = slots[s, my_rows, :]

    def reload(src, e):
        later = e + RING // 2
        if not isinstance(later, int):
            @pl.when(later < experts)
            def _():
                load(src, later).start()
        elif later < experts:
            load(src, later).start()

    def squares(x):
        return jnp.sum(x * x, axis=0, keepdims=True)

    def sums_first(src, e):
        part0[src, e:e + 1, :] = squares(buf[(2 * e + src) % RING])

    def sums_stream(begin, end):
        def one(e, _):
            for src in range(2):
                flow(src, e).wait()
                part1[src, pl.ds(e - FIRST, 1), :] = squares(stream[(2 * (e - FIRST) + src) % STREAM])

                @pl.when(e + STREAM // 2 < experts)
                def _():
                    flow(src, e + STREAM // 2).start()
            return 0
        lax.fori_loop(begin, end, one, 0)

    few, many = stages_of(n)

    def swap(part, got, send, recv):
        return remote(part.at[1 - core], got.at[0], send.at[0], recv.at[0],
                      {"shard": partner(me, n, 1)})

    def passes(stages, s, got, run, send, recv):
        first = 1 + peers_of(stages[:s])
        return [
            remote(run.at[s], got.at[first + i], send.at[first + i], recv.at[first + i],
                   {"shard": partner(me, n, mask)})
            for i, mask in enumerate(stages[s])
        ]

    def share(stages, total, send, recv):
        i = 1 + peers_of(stages)
        return remote(total.at[core], total.at[core], send.at[i], recv.at[i],
                      {"shard": partner(me, n, 1)})

    def swap_end(stages, part, got, run, total, send, recv):
        swap(part, got, send, recv).wait()
        value = part[core] + got[0]
        if stages:
            run[0] = value
        else:
            total[core] = value

    def pass_end(stages, s, got, run, total, send, recv):
        value = run[s]
        for i, copy in enumerate(passes(stages, s, got, run, send, recv)):
            copy.wait()
            value = value + got[1 + peers_of(stages[:s]) + i]
        if s + 1 < len(stages):
            run[s + 1] = value
        else:
            total[core] = value

    def finish(stages, total, begin, end, send, recv):
        share(stages, total, send, recv).wait()
        for src in range(2):
            scale = jnp.sqrt(total[src])
            scales[src, begin:end, :] = scale
            reciprocal = 1.0 / scale
            for j in range(tiles):
                inverse[src, j, begin:end, :] = reciprocal[:, j * LANES:(j + 1) * LANES]

    def mine(x):
        chosen = x[:, :narrow]
        for t in range(1, n):
            chosen = jnp.where(me == t, x[:, t * narrow:(t + 1) * narrow], chosen)
        return chosen

    def first_copy(mask):
        return remote(piece, column.at[:, my_lanes], first_send.at[mask - 1], first_recv.at[mask - 1],
                      {"shard": partner(me, n, mask)})

    my_columns = pl.ds(pl.multiple_of(mez * router_rows, router_rows), router_rows)

    def second_copy(r):
        return remote(column, router_out.at[my_columns, :], second_send.at[r - 1], second_recv.at[r - 1],
                      {"expert": lax.rem(mez + r, nz)})

    def settle(src):
        for mask in range(1, n):
            slab_copy(src, 0, mask, True).wait_recv()
        row = 1.0 / mine(scales[src, 0:1, :])
        pad = -narrow % LANES
        if pad:
            row = jnp.concatenate([row, jnp.zeros((1, pad), jnp.float32)], axis=1)
        factor = jnp.broadcast_to(row, (LANES, narrow + pad)).T[:narrow]

        def tile(j, _):
            lanes = pl.ds(pl.multiple_of(j * LANES, LANES), LANES)
            y = out[src * experts, :, lanes].astype(jnp.float32) * factor
            out[src * experts, :, lanes] = y.astype(jnp.bfloat16)
            return 0

        lax.fori_loop(0, rows * n // LANES, tile, 0)

    last = len(phases) - 1
    half = len(phases) // 2

    load(0, 0).wait()
    narrow_slab(0, 0, raw=True)
    pl.semaphore_wait(barrier, n - 1 + nz - 1)
    for q in range(half):
        phase(0, 0, q)
    sums_first(0, 0)
    for k in range(1, 2 * FIRST):
        load(k % 2, k // 2).wait()
        sums_first(k % 2, k // 2)
    swap(part0, got0, send0, recv0).start()
    reload(0, 0)
    narrow_slab(1, 0, raw=True)
    reload(1, 0)
    swap_end(few, part0, got0, run0, total0, send0, recv0)
    for copy in passes(few, 0, got0, run0, send0, recv0):
        copy.start()

    chunks = [FIRST + (experts - FIRST) * i // 7 for i in range(8)]

    def chunk(i):
        sums_stream(chunks[i], chunks[i + 1])

    def phase_run(k, begin, end):
        for q in range(begin, end):
            phase(k % 2, k // 2, q)

    def ahead(k):
        narrow_slab(k % 2, k // 2)
        reload(k % 2, k // 2)

    phase(0, 0, half)
    weight_load.wait()
    gain_load.wait()
    value = (weight_in[...] * gain_in[...]).astype(jnp.bfloat16)
    piece[...] = value
    column[:, my_lanes] = value
    for mask in range(1, n):
        first_copy(mask).start()
    chunk(0)
    phase_run(0, half + 1, last + 1)
    chunk(1)
    phase(1, 0, 0)
    chunk(2)
    pass_end(few, 0, got0, run0, total0, send0, recv0)
    share(few, total0, send0, recv0).start()
    phase(1, 0, 1)
    chunk(3)
    finish(few, total0, 0, FIRST, send0, recv0)
    phase(1, 0, 2)
    ahead(2)
    phase_run(1, 3, last + 1)
    chunk(4)
    phase(0, 1, 0)
    chunk(5)
    phase(0, 1, 1)
    chunk(6)
    swap(part1, got1, send1, recv1).start()
    ahead(3)
    swap_end(many, part1, got1, run1, total1, send1, recv1)
    for copy in passes(many, 0, got1, run1, send1, recv1):
        copy.start()
    phase_run(2, 2, last + 1)
    phase_run(3, 0, half)
    ahead(4)
    phase_run(3, half, last + 1)
    for s in range(1, len(many)):
        pass_end(many, s - 1, got1, run1, total1, send1, recv1)
        for copy in passes(many, s, got1, run1, send1, recv1):
            copy.start()
    phase_run(4, 0, half)
    ahead(5)
    phase_run(4, half, last + 1)
    for mask in range(1, n):
        first_copy(mask).wait()
    for r in range(1, nz):
        second_copy(r).start()
    router_out[my_columns, :] = column[...]
    pass_end(many, len(many) - 1, got1, run1, total1, send1, recv1)
    share(many, total1, send1, recv1).start()
    phase_run(5, 0, half)
    finish(many, total1, FIRST, experts, send1, recv1)
    ahead(6)
    phase_run(5, half, last + 1)
    for src in range(2):
        settle(src)

    def step(e, _):
        for src in range(2):
            for q in range(half):
                phase(src, e, q)
            if src == 0:
                narrow_slab(1, e)
                reload(1, e)
            else:
                @pl.when(e + 1 < experts)
                def _():
                    narrow_slab(0, e + 1)
                    reload(0, e + 1)
            for q in range(half, last + 1):
                phase(src, e, q)
        return 0

    lax.fori_loop(FIRST, experts, step, 0)

    for ref, src in ((scale_gate, 0), (scale_up, 1)):
        ref[...] = mine(scales[src])
    for r in range(1, nz):
        second_copy(r).wait()
    for q in range(last + 1 - DEPTH, last + 1):
        wait_phase(1, experts - 1, q)
    for mask in range(1, n):
        for src in range(2):
            whole = out.at[src * experts + 1:(src + 1) * experts, :, my_lanes]
            remote(whole, whole, send_sem.at[0, mask - 1], recv_sem.at[src, mask - 1],
                   {"shard": partner(me, n, mask)}).wait_recv()


def deliver(experts, out, scale_gate, scale_up, router,
            to_gate, to_up, to_scale_gate, to_scale_up, to_router, sem):
    copies = [
        pltpu.make_async_copy(source, target, sem.at[i])
        for i, (source, target) in enumerate((
            (out.at[:experts], to_gate), (out.at[experts:], to_up),
            (scale_gate, to_scale_gate), (scale_up, to_scale_up), (router, to_router)))
    ]
    for copy in copies:
        copy.start()
    for copy in copies:
        copy.wait()


def fused(n, nz, master_gate, master_up, router_weight, router_gain):
    experts, rows, width = master_gate.shape
    slabs = 2 * experts
    narrow = width // n
    router_rows = router_weight.shape[1]
    few, many = stages_of(n)
    rest = experts - FIRST
    vmem = pl.BlockSpec(memory_space=pltpu.VMEM)
    hbm = pl.BlockSpec(memory_space=pltpu.HBM)
    dma = pltpu.SemaphoreType.DMA
    f32, bf16 = jnp.float32, jnp.bfloat16

    def sums(count, stages):
        peers = peers_of(stages)
        return [
            pltpu.VMEM((2, count, width), f32),
            pltpu.VMEM((1 + peers, count, width), f32),
            pltpu.VMEM((max(len(stages), 1), count, width), f32),
            pltpu.VMEM((2, count, width), f32),
        ]

    results = pl.pallas_call(
        functools.partial(kernel, n, nz),
        out_shape=(
            pltpu.VMEM((slabs, narrow, rows * n), bf16),
            pltpu.VMEM((experts, narrow), f32),
            pltpu.VMEM((experts, narrow), f32),
            pltpu.VMEM((router_rows * nz, rows * n), bf16),
        ),
        in_specs=[hbm] * 4,
        out_specs=(vmem,) * 4,
        scratch_shapes=[
            pltpu.VMEM((RING, rows, width), f32),
            pltpu.VMEM((STREAM, rows, width), f32),
            pltpu.VMEM((SLOTS, width, rows), bf16),
            *sums(FIRST, few),
            *sums(rest, many),
            pltpu.VMEM((2, experts, width), f32),
            pltpu.VMEM((2, width // LANES, experts, LANES), f32),
            pltpu.VMEM((router_rows, rows), f32),
            pltpu.VMEM((1, rows), f32),
            pltpu.VMEM((router_rows, rows), bf16),
            pltpu.VMEM((router_rows, rows * n), bf16),
            dma((RING,)), dma((STREAM,)), dma((2,)),
            dma((SLOTS, n - 1)), dma((2, n - 1)), dma((2, n - 1)),
            dma((2 + peers_of(few),)), dma((2 + peers_of(few),)),
            dma((2 + peers_of(many),)), dma((2 + peers_of(many),)),
            dma((n - 1,)), dma((n - 1,)), dma((nz - 1,)), dma((nz - 1,)),
        ],
        compiler_params=pltpu.CompilerParams(
            collective_id=0, has_side_effects=True,
            vmem_limit_bytes=VMEM_LIMIT - slabs * narrow * rows * n * 2 - SPARE),
        name="exchange",
    )(master_gate, master_up, router_weight.T, router_gain[None, :])
    final_gate, final_up, scale_gate, scale_up, router = pl.pallas_call(
        functools.partial(deliver, experts),
        out_shape=(
            jax.ShapeDtypeStruct((experts, narrow, rows * n), bf16),
            jax.ShapeDtypeStruct((experts, narrow, rows * n), bf16),
            jax.ShapeDtypeStruct((experts, narrow), f32),
            jax.ShapeDtypeStruct((experts, narrow), f32),
            jax.ShapeDtypeStruct((router_rows * nz, rows * n), bf16),
        ),
        in_specs=[vmem] * 4,
        out_specs=(hbm,) * 5,
        scratch_shapes=[dma((5,))],
        compiler_params=pltpu.CompilerParams(vmem_limit_bytes=1048576),
        name="deliver",
    )(*(pltpu.with_memory_space_constraint(x, pltpu.VMEM) for x in results))
    return (final_gate.swapaxes(1, 2), final_up.swapaxes(1, 2), scale_gate, scale_up, router.T)


def solution(mesh):
    n, nz = mesh.shape["shard"], mesh.shape["expert"]

    def local(master_gate, master_up, router_weight, router_gain):
        experts, rows, width = master_gate.shape
        slabs = 2 * experts
        held = (
            (RING + STREAM) * rows * width * 4 + SLOTS * rows * width * 2
            + slabs * rows * width * 2 + 16 * slabs * width * 4
        )
        fits = (
            n >= 4 and n & (n - 1) == 0 and nz > 1 and held <= VMEM_LIMIT - 2 * SPARE
            and rows % LANES == 0 and width % LANES == 0 and width % (16 * n) == 0
            and experts >= FIRST + 7 and router_weight.shape[1] % 16 == 0
        )
        if not fits:
            return plain(master_gate, master_up, router_weight, router_gain)
        return fused(n, nz, master_gate, master_up, router_weight, router_gain)

    in_specs = (
        P("expert", "shard", None),
        P("expert", "shard", None),
        P("shard", "expert"),
        P("shard"),
    )
    out_specs = (
        P("expert", None, "shard"),
        P("expert", None, "shard"),
        P("expert", "shard"),
        P("expert", "shard"),
        P(),
    )
    return jax.shard_map(local, mesh=mesh, in_specs=in_specs, out_specs=out_specs, check_vma=False)
```

```python
import functools

import jax
import jax.numpy as jnp
from jax import lax
from jax.experimental import pallas as pl
from jax.experimental.pallas import tpu as pltpu
from jax.sharding import PartitionSpec as P

LANES = 128
HELD = 4
STREAM = 6
SLOTS = 4
DEPTH = 3
PHASES = ((6, 1), (2, 4), (7,), (3, 5))
OPENING = (
    ((0, 6, True),),
    ((0, 2, True), (1, 4, True)),
    ((1, 6, True),),
    ((0, 7, False), (0, 1, False)),
    ((0, 3, False), (0, 4, False)),
    ((1, 7, False), (1, 1, False)),
    ((1, 2, False), (1, 5, False)),
    ((1, 3, False), (0, 5, False)),
)
EARLY = ((2, 4, 6),)
LATE = ((2,), (4,))
VMEM_LIMIT = 67043328
SPARE = 4194304

def plain(master_gate, master_up, router_weight, router_gain):
    total_gate, total_up = lax.psum(
        (jnp.sum(master_gate * master_gate, axis=1), jnp.sum(master_up * master_up, axis=1)),
        "shard",
    )
    scale_gate = jnp.sqrt(total_gate)
    scale_up = jnp.sqrt(total_up)
    narrow_gate, narrow_up = (
        (master_gate / jnp.expand_dims(scale_gate, 1)).astype(jnp.bfloat16),
        (master_up / jnp.expand_dims(scale_up, 1)).astype(jnp.bfloat16),
    )
    final_gate, final_up = (
        lax.all_to_all(narrow_gate, "shard", split_axis=2, concat_axis=1, tiled=True),
        lax.all_to_all(narrow_up, "shard", split_axis=2, concat_axis=1, tiled=True),
    )
    scale_gate = lax.dynamic_slice_in_dim(
        scale_gate, lax.axis_index("shard") * final_gate.shape[2], final_gate.shape[2], axis=1
    )
    scale_up = lax.dynamic_slice_in_dim(
        scale_up, lax.axis_index("shard") * final_up.shape[2], final_up.shape[2], axis=1
    )
    part_router = (router_weight * router_gain[:, None]).astype(jnp.bfloat16)
    row_router = lax.all_gather(part_router, "shard", axis=0, tiled=True)
    serve_router = lax.all_gather(row_router, "expert", axis=1, tiled=True)
    return (final_gate, final_up, scale_gate, scale_up, serve_router)


def partner(me, n, mask):
    index, bit = 0, 1
    while bit < n:
        mine = lax.rem(me // bit, 2)
        index = index + bit * (1 - mine if mask & bit else mine)
        bit *= 2
    return index


def peers_of(stages):
    return sum(len(stage) for stage in stages)


def remote(source, target, send, recv, device):
    return pltpu.make_async_remote_copy(
        src_ref=source, dst_ref=target, send_sem=send, recv_sem=recv,
        device_id=device, device_id_type=pl.DeviceIdType.MESH)


def kernel(n, nz, gate, up, weight, gain, out, scale_gate, scale_up, router_out,
           buf, stream, slots, part0, got0, part1, got1, run1, total1, part2, got2, run2, total2,
           scales, inverse, weight_in, gain_in, piece, column,
           load_sem, stream_sem, router_sem, send_sem, recv_sem, raw_sem,
           send0, recv0, send1, recv1, send2, recv2,
           first_send, first_recv, second_send, second_recv):
    me = lax.axis_index("shard")
    mez = lax.axis_index("expert")
    core = lax.rem(me, 2)
    experts, rows, width = gate.shape
    narrow = width // n
    tiles = width // LANES
    router_rows = weight.shape[0]
    sources = (gate, up)
    ring = 2 * HELD

    def load(src, e):
        k = (2 * e + src) % ring
        return pltpu.make_async_copy(sources[src].at[e], buf.at[k], load_sem.at[k])

    def flow(src, e):
        k = (2 * (e - HELD) + src) % STREAM
        return pltpu.make_async_copy(sources[src].at[e], stream.at[k], stream_sem.at[k])

    for e in range(HELD):
        for src in range(2):
            load(src, e).start()
    weight_load = pltpu.make_async_copy(weight, weight_in, router_sem.at[0])
    gain_load = pltpu.make_async_copy(gain, gain_in, router_sem.at[1])
    weight_load.start()
    gain_load.start()
    for e in range(HELD, HELD + STREAM // 2):
        for src in range(2):
            flow(src, e).start()

    barrier = pltpu.get_barrier_semaphore()
    for mask in range(1, n):
        pl.semaphore_signal(barrier, inc=1, device_id={"shard": partner(me, n, mask)},
                            device_id_type=pl.DeviceIdType.MESH)
    for r in range(1, nz):
        pl.semaphore_signal(barrier, inc=1, device_id={"expert": lax.rem(mez + r, nz)},
                            device_id_type=pl.DeviceIdType.MESH)

    my_lanes = pl.ds(pl.multiple_of(me * rows, rows), rows)
    my_rows = pl.ds(pl.multiple_of(me * narrow, 16), narrow)

    def slab_copy(src, e, mask, raw):
        s = 2 + src if raw else (2 * e + src) % SLOTS
        target = partner(me, n, mask)
        return remote(
            slots.at[s, pl.ds(pl.multiple_of(target * narrow, 16), narrow), :],
            out.at[src * experts + e, :, my_lanes],
            send_sem.at[s, mask - 1], (raw_sem if raw else recv_sem).at[src, mask - 1],
            {"shard": target})

    def units(src, e, q):
        if isinstance(e, int) and e == 0:
            return OPENING[len(PHASES) * src + q]
        return [(src, mask, False) for mask in PHASES[q]]

    def wait_phase(src, e, q):
        for which, mask, raw in units(src, e, q):
            slab_copy(which, e, mask, raw).wait_send()

    def phase(src, e, q):
        back, before = q - DEPTH, src
        while back < 0:
            back += len(PHASES)
            before -= 1
        lag = e + before // 2
        if not isinstance(lag, int) or lag >= 0:
            wait_phase(before % 2, lag, back)
        for which, mask, raw in units(src, e, q):
            slab_copy(which, e, mask, raw).start()

    def raw_block(src, mask):
        begin = partner(me, n, mask) * narrow

        def tile(j, _):
            lanes = pl.ds(pl.multiple_of(j * LANES, LANES), LANES)
            slots[2 + src, lanes, :] = buf[src, :, lanes].T.astype(jnp.bfloat16)
            return 0

        lax.fori_loop(begin // LANES, (begin + narrow - 1) // LANES + 1, tile, 0)

    def narrow_slab(src, e):
        k = 2 * e + src
        b, s = k % ring, k % SLOTS
        if not isinstance(e, int) or e >= HELD:
            load(src, e).wait()

        def tile(j, _):
            lanes = pl.ds(pl.multiple_of(j * LANES, LANES), LANES)
            y = buf[b, :, lanes] * inverse[src, j, pl.ds(e, 1), :]
            slots[s, lanes, :] = y.T.astype(jnp.bfloat16)
            return 0

        lax.fori_loop(0, tiles, tile, 0)
        out[src * experts + e, :, my_lanes] = slots[s, my_rows, :]
        if isinstance(e, int):
            if e + HELD < experts:
                load(src, e + HELD).start()
        else:
            @pl.when(e + HELD < experts)
            def _():
                load(src, e + HELD).start()

    def squares(x):
        return jnp.sum(x * x, axis=0, keepdims=True)

    def sums_held(src, e):
        load(src, e).wait()
        value = squares(buf[2 * e + src])
        if e == 0:
            part0[src] = value
        else:
            part1[src, e - 1:e, :] = value

    def sums_stream(begin, end):
        def one(e, _):
            for src in range(2):
                flow(src, e).wait()
                part2[src, pl.ds(e - HELD, 1), :] = squares(stream[(2 * (e - HELD) + src) % STREAM])

                @pl.when(e + STREAM // 2 < experts)
                def _():
                    flow(src, e + STREAM // 2).start()
            return 0
        lax.fori_loop(begin, end, one, 0)

    def keep(src, begin, end, total):
        scale = jnp.sqrt(total)
        scales[src, begin:end, :] = scale
        reciprocal = 1.0 / scale
        for j in range(tiles):
            inverse[src, j, begin:end, :] = reciprocal[:, j * LANES:(j + 1) * LANES]

    def greet(mask):
        return remote(part0, got0.at[mask - 1], send0.at[mask - 1], recv0.at[mask - 1],
                      {"shard": partner(me, n, mask)})

    def greet_end():
        for mask in range(1, n):
            greet(mask).wait()
        for src in range(2):
            total = part0[src]
            for mask in range(1, n):
                total = total + got0[mask - 1, src]
            keep(src, 0, 1, total)

    class Sums:
        def __init__(self, stages, begin, end, part, got, run, total, send, recv):
            self.stages, self.begin, self.end = stages, begin, end
            self.part, self.got, self.run, self.total = part, got, run, total
            self.send, self.recv = send, recv

        def copy(self, source, target, i, mask):
            return remote(source, target, self.send.at[i], self.recv.at[i],
                          {"shard": partner(me, n, mask)})

        def swap(self):
            return self.copy(self.part.at[1 - core], self.got.at[0], 0, 1)

        def swap_end(self):
            self.swap().wait()
            self.run[0] = self.part[core] + self.got[0]

        def passes(self, s):
            first = 1 + peers_of(self.stages[:s])
            return [self.copy(self.run.at[s], self.got.at[first + i], first + i, mask)
                    for i, mask in enumerate(self.stages[s])]

        def pass_start(self, s):
            for copy in self.passes(s):
                copy.start()

        def pass_end(self, s):
            value = self.run[s]
            for i, copy in enumerate(self.passes(s)):
                copy.wait()
                value = value + self.got[1 + peers_of(self.stages[:s]) + i]
            if s + 1 < len(self.stages):
                self.run[s + 1] = value
            else:
                self.total[core] = value

        def share(self):
            half = self.total.at[core]
            return self.copy(half, half, 1 + peers_of(self.stages), 1)

        def finish(self):
            self.share().wait()
            for src in range(2):
                keep(src, self.begin, self.end, self.total[src])

    early = Sums(EARLY, 1, HELD, part1, got1, run1, total1, send1, recv1)
    late = Sums(LATE, HELD, experts, part2, got2, run2, total2, send2, recv2)

    def mine(x):
        chosen = x[:, :narrow]
        for t in range(1, n):
            chosen = jnp.where(me == t, x[:, t * narrow:(t + 1) * narrow], chosen)
        return chosen

    def first_copy(mask):
        return remote(piece, column.at[:, my_lanes], first_send.at[mask - 1], first_recv.at[mask - 1],
                      {"shard": partner(me, n, mask)})

    my_columns = pl.ds(pl.multiple_of(mez * router_rows, router_rows), router_rows)

    def second_copy(r):
        return remote(column, router_out.at[my_columns, :], second_send.at[r - 1], second_recv.at[r - 1],
                      {"expert": lax.rem(mez + r, nz)})

    raw_units = [(src, mask) for group in OPENING for src, mask, raw in group if raw]

    def settle(src):
        row = 1.0 / mine(scales[src, 0:1, :])
        pad = -narrow % LANES
        if pad:
            row = jnp.concatenate([row, jnp.zeros((1, pad), jnp.float32)], axis=1)
        factor = jnp.broadcast_to(row, (LANES, narrow + pad)).T[:narrow]
        for which, mask in raw_units:
            if which != src:
                continue
            slab_copy(src, 0, mask, True).wait_recv()
            begin = partner(me, n, mask) * rows
            for j in range(rows // LANES):
                lanes = pl.ds(pl.multiple_of(begin + j * LANES, LANES), LANES)
                y = out[src * experts, :, lanes].astype(jnp.float32) * factor
                out[src * experts, :, lanes] = y.astype(jnp.bfloat16)

    last = len(PHASES)
    half = last // 2
    steps = experts - HELD
    cuts = [HELD + steps * i // 6 for i in range(7)]

    def chunk(i):
        sums_stream(cuts[i], cuts[i + 1])

    def run(k, begin, end):
        for q in range(begin, end):
            phase(k % 2, k // 2, q)

    def ahead(k):
        narrow_slab(k % 2, k // 2)

    sums_held(0, 0)
    sums_held(1, 0)
    raw_block(0, 6)
    pl.semaphore_wait(barrier, n - 1 + nz - 1)
    for mask in range(1, n):
        greet(mask).start()
    run(0, 0, 1)
    raw_block(0, 2)
    raw_block(1, 4)
    run(0, 1, 2)
    raw_block(1, 6)
    run(0, 2, 3)
    for e in range(1, HELD):
        for src in range(2):
            sums_held(src, e)
    early.swap().start()
    greet_end()
    ahead(0)
    run(0, 3, 4)
    run(1, 0, 1)
    early.swap_end()
    early.pass_start(0)
    ahead(1)
    run(1, 1, 2)
    weight_load.wait()
    gain_load.wait()
    value = (weight_in[...] * gain_in[...]).astype(jnp.bfloat16)
    piece[...] = value
    column[:, my_lanes] = value
    for mask in range(1, n):
        first_copy(mask).start()
    chunk(0)
    run(1, 2, 3)
    chunk(1)
    early.pass_end(0)
    early.share().start()
    run(1, 3, 4)
    chunk(2)
    early.finish()
    ahead(2)
    run(2, 0, 1)
    chunk(3)
    run(2, 1, 2)
    ahead(3)
    run(2, 2, 3)
    chunk(4)
    run(2, 3, 4)
    chunk(5)
    late.swap().start()
    run(3, 0, 1)
    late.swap_end()
    late.pass_start(0)
    run(3, 1, half)
    ahead(4)
    run(3, half, last)
    run(4, 0, half)
    late.pass_end(0)
    late.pass_start(1)
    ahead(5)
    run(4, half, last)
    run(5, 0, half)
    late.pass_end(1)
    late.share().start()
    ahead(6)
    run(5, half, last)
    late.finish()
    run(6, 0, half)
    ahead(7)
    for src in range(2):
        settle(src)
    run(6, half, last)
    for mask in range(1, n):
        first_copy(mask).wait()
    for r in range(1, nz):
        second_copy(r).start()
    router_out[my_columns, :] = column[...]
    run(7, 0, half)
    ahead(8)
    run(7, half, last)

    def step(e, _):
        for src in range(2):
            for q in range(half):
                phase(src, e, q)
            if src == 0:
                narrow_slab(1, e)
            else:
                @pl.when(e + 1 < experts)
                def _():
                    narrow_slab(0, e + 1)
            for q in range(half, last):
                phase(src, e, q)
        return 0

    lax.fori_loop(HELD, experts, step, 0)

    for ref, src in ((scale_gate, 0), (scale_up, 1)):
        ref[...] = mine(scales[src])
    for r in range(1, nz):
        second_copy(r).wait()
    for q in range(last - DEPTH, last):
        wait_phase(1, experts - 1, q)
    for mask in range(1, n):
        for src in range(2):
            begin = src * experts + (1 if (src, mask) in raw_units else 0)
            whole = out.at[begin:(src + 1) * experts, :, my_lanes]
            remote(whole, whole, send_sem.at[0, mask - 1], recv_sem.at[src, mask - 1],
                   {"shard": partner(me, n, mask)}).wait_recv()


def deliver(experts, out, scale_gate, scale_up, router,
            to_gate, to_up, to_scale_gate, to_scale_up, to_router, sem):
    copies = [
        pltpu.make_async_copy(source, target, sem.at[i])
        for i, (source, target) in enumerate((
            (out.at[:experts], to_gate), (out.at[experts:], to_up),
            (scale_gate, to_scale_gate), (scale_up, to_scale_up), (router, to_router)))
    ]
    for copy in copies:
        copy.start()
    for copy in copies:
        copy.wait()


def fused(n, nz, master_gate, master_up, router_weight, router_gain):
    experts, rows, width = master_gate.shape
    slabs = 2 * experts
    narrow = width // n
    router_rows = router_weight.shape[1]
    vmem = pl.BlockSpec(memory_space=pltpu.VMEM)
    hbm = pl.BlockSpec(memory_space=pltpu.HBM)
    dma = pltpu.SemaphoreType.DMA
    f32, bf16 = jnp.float32, jnp.bfloat16

    def sums(count, stages):
        peers = peers_of(stages)
        return [
            pltpu.VMEM((2, count, width), f32),
            pltpu.VMEM((1 + peers, count, width), f32),
            pltpu.VMEM((len(stages), count, width), f32),
            pltpu.VMEM((2, count, width), f32),
        ]

    results = pl.pallas_call(
        functools.partial(kernel, n, nz),
        out_shape=(
            pltpu.VMEM((slabs, narrow, rows * n), bf16),
            pltpu.VMEM((experts, narrow), f32),
            pltpu.VMEM((experts, narrow), f32),
            pltpu.VMEM((router_rows * nz, rows * n), bf16),
        ),
        in_specs=[hbm] * 4,
        out_specs=(vmem,) * 4,
        scratch_shapes=[
            pltpu.VMEM((2 * HELD, rows, width), f32),
            pltpu.VMEM((STREAM, rows, width), f32),
            pltpu.VMEM((SLOTS, width, rows), bf16),
            pltpu.VMEM((2, 1, width), f32),
            pltpu.VMEM((n - 1, 2, 1, width), f32),
            *sums(HELD - 1, EARLY),
            *sums(experts - HELD, LATE),
            pltpu.VMEM((2, experts, width), f32),
            pltpu.VMEM((2, width // LANES, experts, LANES), f32),
            pltpu.VMEM((router_rows, rows), f32),
            pltpu.VMEM((1, rows), f32),
            pltpu.VMEM((router_rows, rows), bf16),
            pltpu.VMEM((router_rows, rows * n), bf16),
            dma((2 * HELD,)), dma((STREAM,)), dma((2,)),
            dma((SLOTS, n - 1)), dma((2, n - 1)), dma((2, n - 1)),
            dma((n - 1,)), dma((n - 1,)),
            dma((2 + peers_of(EARLY),)), dma((2 + peers_of(EARLY),)),
            dma((2 + peers_of(LATE),)), dma((2 + peers_of(LATE),)),
            dma((n - 1,)), dma((n - 1,)), dma((nz - 1,)), dma((nz - 1,)),
        ],
        compiler_params=pltpu.CompilerParams(
            collective_id=0, has_side_effects=True,
            vmem_limit_bytes=VMEM_LIMIT - slabs * narrow * rows * n * 2 - SPARE),
        name="exchange",
    )(master_gate, master_up, router_weight.T, router_gain[None, :])
    final_gate, final_up, scale_gate, scale_up, router = pl.pallas_call(
        functools.partial(deliver, experts),
        out_shape=(
            jax.ShapeDtypeStruct((experts, narrow, rows * n), bf16),
            jax.ShapeDtypeStruct((experts, narrow, rows * n), bf16),
            jax.ShapeDtypeStruct((experts, narrow), f32),
            jax.ShapeDtypeStruct((experts, narrow), f32),
            jax.ShapeDtypeStruct((router_rows * nz, rows * n), bf16),
        ),
        in_specs=[vmem] * 4,
        out_specs=(hbm,) * 5,
        scratch_shapes=[dma((5,))],
        compiler_params=pltpu.CompilerParams(vmem_limit_bytes=1048576),
        name="deliver",
    )(*(pltpu.with_memory_space_constraint(x, pltpu.VMEM) for x in results))
    return (final_gate.swapaxes(1, 2), final_up.swapaxes(1, 2), scale_gate, scale_up, router.T)


def solution(mesh):
    n, nz = mesh.shape["shard"], mesh.shape["expert"]

    def local(master_gate, master_up, router_weight, router_gain):
        experts, rows, width = master_gate.shape
        slabs = 2 * experts
        held = (
            (2 * HELD + STREAM) * rows * width * 4 + SLOTS * rows * width * 2
            + slabs * rows * width * 2 + 16 * slabs * width * 4
        )
        fits = (
            n == 8 and nz > 1 and held <= VMEM_LIMIT - 2 * SPARE
            and rows % LANES == 0 and width % LANES == 0 and width % (16 * n) == 0
            and experts >= HELD + 6 and router_weight.shape[1] % 16 == 0
        )
        if not fits:
            return plain(master_gate, master_up, router_weight, router_gain)
        return fused(n, nz, master_gate, master_up, router_weight, router_gain)

    in_specs = (
        P("expert", "shard", None),
        P("expert", "shard", None),
        P("shard", "expert"),
        P("shard"),
    )
    out_specs = (
        P("expert", None, "shard"),
        P("expert", None, "shard"),
        P("expert", "shard"),
        P("expert", "shard"),
        P(),
    )
    return jax.shard_map(local, mesh=mesh, in_specs=in_specs, out_specs=out_specs, check_vma=False)
```

```python
import functools

import jax
import jax.numpy as jnp
from jax import lax
from jax.experimental import pallas as pl
from jax.experimental.pallas import tpu as pltpu
from jax.sharding import PartitionSpec as P

LANES = 128
HELD = 4
STREAM = 6
SLOTS = 4
DEPTH = 3
PHASES = ((6, 1), (2, 4), (7,), (3, 5))
OPENING = (
    ((0, 6, True),),
    ((0, 2, True), (1, 4, True)),
    ((1, 6, True),),
    ((0, 7, False), (0, 1, False)),
    ((0, 3, False), (0, 4, False)),
    ((1, 7, False), (1, 1, False)),
    ((1, 2, False), (1, 5, False)),
    ((1, 3, False), (0, 5, False)),
)
EARLY = ((2, 4, 6),)
LATE = ((2,), (4,))
VMEM_LIMIT = 67043328
SPARE = 4194304

def plain(master_gate, master_up, router_weight, router_gain):
    total_gate, total_up = lax.psum(
        (jnp.sum(master_gate * master_gate, axis=1), jnp.sum(master_up * master_up, axis=1)),
        "shard",
    )
    scale_gate = jnp.sqrt(total_gate)
    scale_up = jnp.sqrt(total_up)
    narrow_gate, narrow_up = (
        (master_gate / jnp.expand_dims(scale_gate, 1)).astype(jnp.bfloat16),
        (master_up / jnp.expand_dims(scale_up, 1)).astype(jnp.bfloat16),
    )
    final_gate, final_up = (
        lax.all_to_all(narrow_gate, "shard", split_axis=2, concat_axis=1, tiled=True),
        lax.all_to_all(narrow_up, "shard", split_axis=2, concat_axis=1, tiled=True),
    )
    scale_gate = lax.dynamic_slice_in_dim(
        scale_gate, lax.axis_index("shard") * final_gate.shape[2], final_gate.shape[2], axis=1
    )
    scale_up = lax.dynamic_slice_in_dim(
        scale_up, lax.axis_index("shard") * final_up.shape[2], final_up.shape[2], axis=1
    )
    part_router = (router_weight * router_gain[:, None]).astype(jnp.bfloat16)
    row_router = lax.all_gather(part_router, "shard", axis=0, tiled=True)
    serve_router = lax.all_gather(row_router, "expert", axis=1, tiled=True)
    return (final_gate, final_up, scale_gate, scale_up, serve_router)


def partner(me, n, mask):
    index, bit = 0, 1
    while bit < n:
        mine = lax.rem(me // bit, 2)
        index = index + bit * (1 - mine if mask & bit else mine)
        bit *= 2
    return index


def peers_of(stages):
    return sum(len(stage) for stage in stages)


def remote(source, target, send, recv, device):
    return pltpu.make_async_remote_copy(
        src_ref=source, dst_ref=target, send_sem=send, recv_sem=recv,
        device_id=device, device_id_type=pl.DeviceIdType.MESH)


def kernel(n, nz, gate, up, weight, gain, out, scale_gate, scale_up, router_out,
           buf, stream, slots, part0, got0, part1, got1, run1, total1, part2, got2, run2, total2,
           scales, inverse, weight_in, gain_in, piece, column,
           load_sem, stream_sem, router_sem, send_sem, recv_sem, raw_sem,
           send0, recv0, send1, recv1, send2, recv2,
           first_send, first_recv, second_send, second_recv, third_send, third_recv, go):
    me = lax.axis_index("shard")
    mez = lax.axis_index("expert")
    core = lax.rem(me, 2)
    experts, rows, width = gate.shape
    narrow = width // n
    tiles = width // LANES
    router_rows = weight.shape[0]
    sources = (gate, up)
    ring = 2 * HELD

    def load(src, e):
        k = (2 * e + src) % ring
        return pltpu.make_async_copy(sources[src].at[e], buf.at[k], load_sem.at[k])

    def flow(src, e):
        k = (2 * (e - HELD) + src) % STREAM
        return pltpu.make_async_copy(sources[src].at[e], stream.at[k], stream_sem.at[k])

    for e in range(HELD):
        for src in range(2):
            load(src, e).start()
    weight_load = pltpu.make_async_copy(weight, weight_in, router_sem.at[0])
    gain_load = pltpu.make_async_copy(gain, gain_in, router_sem.at[1])
    weight_load.start()
    gain_load.start()
    for e in range(HELD, HELD + STREAM // 2):
        for src in range(2):
            flow(src, e).start()

    barrier = pltpu.get_barrier_semaphore()
    for chip in range(n // 2):
        @pl.when(me != 2 * chip)
        def _():
            pl.semaphore_signal(barrier, inc=1, device_id={"shard": 2 * chip},
                                device_id_type=pl.DeviceIdType.MESH)

    @pl.when(core == 1)
    def _():
        for r in range(1, nz):
            pl.semaphore_signal(barrier, inc=1, device_id={"expert": lax.rem(mez + r, nz)},
                                device_id_type=pl.DeviceIdType.MESH)

    @pl.when(core == 0)
    def _():
        pl.semaphore_wait(barrier, n - 1)
        pl.semaphore_signal(go, inc=1, device_id={"shard": partner(me, n, 1)},
                            device_id_type=pl.DeviceIdType.MESH)

    def greeted():
        @pl.when(core == 1)
        def _():
            pl.semaphore_wait(go, 1)

    my_lanes = pl.ds(pl.multiple_of(me * rows, rows), rows)
    my_rows = pl.ds(pl.multiple_of(me * narrow, 16), narrow)

    def slab_copy(src, e, mask, raw):
        s = 2 + src if raw else (2 * e + src) % SLOTS
        target = partner(me, n, mask)
        return remote(
            slots.at[s, pl.ds(pl.multiple_of(target * narrow, 16), narrow), :],
            out.at[src * experts + e, :, my_lanes],
            send_sem.at[s, mask - 1], (raw_sem if raw else recv_sem).at[src, mask - 1],
            {"shard": target})

    def units(src, e, q):
        if isinstance(e, int) and e == 0:
            return OPENING[len(PHASES) * src + q]
        return [(src, mask, False) for mask in PHASES[q]]

    def wait_phase(src, e, q):
        for which, mask, raw in units(src, e, q):
            slab_copy(which, e, mask, raw).wait_send()

    def phase(src, e, q):
        back, before = q - DEPTH, src
        while back < 0:
            back += len(PHASES)
            before -= 1
        lag = e + before // 2
        if not isinstance(lag, int) or lag >= 0:
            wait_phase(before % 2, lag, back)
        for which, mask, raw in units(src, e, q):
            slab_copy(which, e, mask, raw).start()

    def raw_block(src, mask):
        begin = partner(me, n, mask) * narrow

        def tile(j, _):
            lanes = pl.ds(pl.multiple_of(j * LANES, LANES), LANES)
            slots[2 + src, lanes, :] = buf[src, :, lanes].T.astype(jnp.bfloat16)
            return 0

        lax.fori_loop(begin // LANES, (begin + narrow - 1) // LANES + 1, tile, 0)

    def narrow_slab(src, e):
        k = 2 * e + src
        b, s = k % ring, k % SLOTS
        if not isinstance(e, int) or e >= HELD:
            load(src, e).wait()

        def tile(j, _):
            lanes = pl.ds(pl.multiple_of(j * LANES, LANES), LANES)
            y = buf[b, :, lanes] * inverse[src, j, pl.ds(e, 1), :]
            slots[s, lanes, :] = y.T.astype(jnp.bfloat16)
            return 0

        lax.fori_loop(0, tiles, tile, 0, unroll=True)
        out[src * experts + e, :, my_lanes] = slots[s, my_rows, :]
        if isinstance(e, int):
            if e + HELD < experts:
                load(src, e + HELD).start()
        else:
            @pl.when(e + HELD < experts)
            def _():
                load(src, e + HELD).start()

    def squares(x):
        return jnp.sum(x * x, axis=0, keepdims=True)

    def sums_held(src, e):
        load(src, e).wait()
        value = squares(buf[2 * e + src])
        if e == 0:
            part0[src] = value
        else:
            part1[src, e - 1:e, :] = value

    def sums_stream(begin, end):
        def one(e, _):
            for src in range(2):
                flow(src, e).wait()
                part2[src, pl.ds(e - HELD, 1), :] = squares(stream[(2 * (e - HELD) + src) % STREAM])

                @pl.when(e + STREAM // 2 < experts)
                def _():
                    flow(src, e + STREAM // 2).start()
            return 0
        lax.fori_loop(begin, end, one, 0)

    def keep(src, begin, end, total):
        scale = jnp.sqrt(total)
        scales[src, begin:end, :] = scale
        reciprocal = 1.0 / scale
        for j in range(tiles):
            inverse[src, j, begin:end, :] = reciprocal[:, j * LANES:(j + 1) * LANES]

    def greet(mask):
        return remote(part0, got0.at[mask - 1], send0.at[mask - 1], recv0.at[mask - 1],
                      {"shard": partner(me, n, mask)})

    def greet_end():
        for mask in range(1, n):
            greet(mask).wait()
        for src in range(2):
            total = part0[src]
            for mask in range(1, n):
                total = total + got0[mask - 1, src]
            keep(src, 0, 1, total)

    class Sums:
        def __init__(self, stages, begin, end, part, got, run, total, send, recv):
            self.stages, self.begin, self.end = stages, begin, end
            self.part, self.got, self.run, self.total = part, got, run, total
            self.send, self.recv = send, recv

        def copy(self, source, target, i, mask):
            return remote(source, target, self.send.at[i], self.recv.at[i],
                          {"shard": partner(me, n, mask)})

        def swap(self):
            return self.copy(self.part.at[1 - core], self.got.at[0], 0, 1)

        def swap_end(self):
            self.swap().wait()
            self.run[0] = self.part[core] + self.got[0]

        def passes(self, s):
            first = 1 + peers_of(self.stages[:s])
            return [self.copy(self.run.at[s], self.got.at[first + i], first + i, mask)
                    for i, mask in enumerate(self.stages[s])]

        def pass_start(self, s):
            for copy in self.passes(s):
                copy.start()

        def pass_end(self, s):
            value = self.run[s]
            for i, copy in enumerate(self.passes(s)):
                copy.wait()
                value = value + self.got[1 + peers_of(self.stages[:s]) + i]
            if s + 1 < len(self.stages):
                self.run[s + 1] = value
            else:
                self.total[core] = value

        def share(self):
            half = self.total.at[core]
            return self.copy(half, half, 1 + peers_of(self.stages), 1)

        def finish(self):
            self.share().wait()
            for src in range(2):
                keep(src, self.begin, self.end, self.total[src])

    early = Sums(EARLY, 1, HELD, part1, got1, run1, total1, send1, recv1)
    late = Sums(LATE, HELD, experts, part2, got2, run2, total2, send2, recv2)

    def mine(x):
        chosen = x[:, :narrow]
        for t in range(1, n):
            chosen = jnp.where(me == t, x[:, t * narrow:(t + 1) * narrow], chosen)
        return chosen

    def first_copy(mask):
        return remote(piece, column.at[:, my_lanes], first_send.at[mask - 1], first_recv.at[mask - 1],
                      {"shard": partner(me, n, mask)})

    my_columns = pl.ds(pl.multiple_of(mez * router_rows, router_rows), router_rows)

    def second_copy(r):
        return remote(column, router_out.at[my_columns, :], second_send.at[r - 1], second_recv.at[r - 1],
                      {"expert": lax.rem(mez + r, nz)})

    def third_copy(r):
        theirs = pl.ds(pl.multiple_of(lax.rem(mez + r, nz) * router_rows, router_rows), router_rows)
        return remote(router_out.at[theirs, :], router_out.at[theirs, :],
                      third_send.at[r - 1], third_recv.at[r - 1], {"shard": partner(me, n, 1)})

    raw_units = [(src, mask) for group in OPENING for src, mask, raw in group if raw]

    def settle(src):
        row = 1.0 / mine(scales[src, 0:1, :])
        pad = -narrow % LANES
        if pad:
            row = jnp.concatenate([row, jnp.zeros((1, pad), jnp.float32)], axis=1)
        factor = jnp.broadcast_to(row, (LANES, narrow + pad)).T[:narrow]
        for which, mask in raw_units:
            if which != src:
                continue
            slab_copy(src, 0, mask, True).wait_recv()
            begin = partner(me, n, mask) * rows
            for j in range(rows // LANES):
                lanes = pl.ds(pl.multiple_of(begin + j * LANES, LANES), LANES)
                y = out[src * experts, :, lanes].astype(jnp.float32) * factor
                out[src * experts, :, lanes] = y.astype(jnp.bfloat16)

    last = len(PHASES)
    half = last // 2
    steps = experts - HELD
    cuts = [HELD + steps * i // 6 for i in range(7)]

    def chunk(i):
        sums_stream(cuts[i], cuts[i + 1])

    def run(k, begin, end):
        for q in range(begin, end):
            phase(k % 2, k // 2, q)

    def ahead(k):
        narrow_slab(k % 2, k // 2)

    sums_held(0, 0)
    sums_held(1, 0)
    raw_block(0, 6)
    greeted()
    for mask in range(1, n):
        greet(mask).start()
    run(0, 0, 1)
    raw_block(0, 2)
    raw_block(1, 4)
    run(0, 1, 2)
    raw_block(1, 6)
    run(0, 2, 3)
    for e in range(1, HELD):
        for src in range(2):
            sums_held(src, e)
    early.swap().start()
    greet_end()
    ahead(0)
    early.swap_end()
    early.pass_start(0)
    run(0, 3, 4)
    run(1, 0, 1)
    ahead(1)
    run(1, 1, 2)
    weight_load.wait()
    gain_load.wait()
    value = (weight_in[...] * gain_in[...]).astype(jnp.bfloat16)
    piece[...] = value
    column[:, my_lanes] = value
    for mask in range(1, n):
        first_copy(mask).start()
    chunk(0)
    run(1, 2, 3)
    chunk(1)
    early.pass_end(0)
    early.share().start()
    run(1, 3, 4)
    early.finish()
    ahead(2)
    run(2, 0, 1)
    chunk(2)
    chunk(3)
    run(2, 1, 2)
    ahead(3)
    run(2, 2, 3)
    chunk(4)
    run(2, 3, 4)
    chunk(5)
    late.swap().start()
    run(3, 0, 1)
    late.swap_end()
    late.pass_start(0)
    run(3, 1, half)
    ahead(4)
    run(3, half, last)
    run(4, 0, half)
    late.pass_end(0)
    late.pass_start(1)
    ahead(5)
    run(4, half, last)
    run(5, 0, half)
    late.pass_end(1)
    late.share().start()
    ahead(6)
    run(5, half, last)
    late.finish()
    run(6, 0, half)
    ahead(7)
    for src in range(2):
        settle(src)
    run(6, half, last)
    for mask in range(1, n):
        first_copy(mask).wait()
    router_out[my_columns, :] = column[...]

    @pl.when(core == 1)
    def _():
        pl.semaphore_wait(barrier, nz - 1)
        for r in range(1, nz):
            second_copy(r).start()

    run(7, 0, half)
    ahead(8)
    run(7, half, last)

    @pl.when(core == 1)
    def _():
        for r in range(1, nz):
            second_copy(r).wait()
        for r in range(1, nz):
            third_copy(r).start()

    run(8, 0, half)
    ahead(9)
    run(8, half, last)
    run(9, 0, half)
    ahead(10)
    run(9, half, last)

    @pl.when(core == 1)
    def _():
        for r in range(1, nz):
            third_copy(r).wait_send()

    def step(e, _):
        for src in range(2):
            for q in range(half):
                phase(src, e, q)
            if src == 0:
                narrow_slab(1, e)
            else:
                @pl.when(e + 1 < experts)
                def _():
                    narrow_slab(0, e + 1)
            for q in range(half, last):
                phase(src, e, q)
        return 0

    lax.fori_loop(HELD + 1, experts, step, 0)

    for ref, src in ((scale_gate, 0), (scale_up, 1)):
        ref[...] = mine(scales[src])

    @pl.when(core == 0)
    def _():
        for r in range(1, nz):
            third_copy(r).wait_recv()

    for q in range(2 * last - DEPTH, 2 * last):
        wait_phase(q // last, experts - 1, q % last)
    for mask in range(1, n):
        for src in range(2):
            begin = src * experts + (1 if (src, mask) in raw_units else 0)
            whole = out.at[begin:(src + 1) * experts, :, my_lanes]
            remote(whole, whole, send_sem.at[0, mask - 1], recv_sem.at[src, mask - 1],
                   {"shard": partner(me, n, mask)}).wait_recv()


def deliver(experts, out, scale_gate, scale_up, router,
            to_gate, to_up, to_scale_gate, to_scale_up, to_router, sem):
    pairs = [(scale_gate, to_scale_gate), (scale_up, to_scale_up), (router, to_router)]
    for e in range(experts):
        pairs += [(out.at[e], to_gate.at[e]), (out.at[experts + e], to_up.at[e])]
    copies = [pltpu.make_async_copy(a, b, sem.at[i]) for i, (a, b) in enumerate(pairs)]
    for copy in copies:
        copy.start()
    for copy in copies:
        copy.wait()


def fused(n, nz, master_gate, master_up, router_weight, router_gain):
    experts, rows, width = master_gate.shape
    slabs = 2 * experts
    narrow = width // n
    router_rows = router_weight.shape[1]
    vmem = pl.BlockSpec(memory_space=pltpu.VMEM)
    hbm = pl.BlockSpec(memory_space=pltpu.HBM)
    dma = pltpu.SemaphoreType.DMA
    f32, bf16 = jnp.float32, jnp.bfloat16

    def sums(count, stages):
        peers = peers_of(stages)
        return [
            pltpu.VMEM((2, count, width), f32),
            pltpu.VMEM((1 + peers, count, width), f32),
            pltpu.VMEM((len(stages), count, width), f32),
            pltpu.VMEM((2, count, width), f32),
        ]

    results = pl.pallas_call(
        functools.partial(kernel, n, nz),
        out_shape=(
            pltpu.VMEM((slabs, narrow, rows * n), bf16),
            pltpu.VMEM((experts, narrow), f32),
            pltpu.VMEM((experts, narrow), f32),
            pltpu.VMEM((router_rows * nz, rows * n), bf16),
        ),
        in_specs=[hbm] * 4,
        out_specs=(vmem,) * 4,
        scratch_shapes=[
            pltpu.VMEM((2 * HELD, rows, width), f32),
            pltpu.VMEM((STREAM, rows, width), f32),
            pltpu.VMEM((SLOTS, width, rows), bf16),
            pltpu.VMEM((2, 1, width), f32),
            pltpu.VMEM((n - 1, 2, 1, width), f32),
            *sums(HELD - 1, EARLY),
            *sums(experts - HELD, LATE),
            pltpu.VMEM((2, experts, width), f32),
            pltpu.VMEM((2, width // LANES, experts, LANES), f32),
            pltpu.VMEM((router_rows, rows), f32),
            pltpu.VMEM((1, rows), f32),
            pltpu.VMEM((router_rows, rows), bf16),
            pltpu.VMEM((router_rows, rows * n), bf16),
            dma((2 * HELD,)), dma((STREAM,)), dma((2,)),
            dma((SLOTS, n - 1)), dma((2, n - 1)), dma((2, n - 1)),
            dma((n - 1,)), dma((n - 1,)),
            dma((2 + peers_of(EARLY),)), dma((2 + peers_of(EARLY),)),
            dma((2 + peers_of(LATE),)), dma((2 + peers_of(LATE),)),
            dma((n - 1,)), dma((n - 1,)), dma((nz - 1,)), dma((nz - 1,)),
            dma((nz - 1,)), dma((nz - 1,)), pltpu.SemaphoreType.REGULAR,
        ],
        compiler_params=pltpu.CompilerParams(
            collective_id=0, has_side_effects=True,
            vmem_limit_bytes=VMEM_LIMIT - slabs * narrow * rows * n * 2 - SPARE),
        name="exchange",
    )(master_gate, master_up, router_weight.T, router_gain[None, :])
    final_gate, final_up, scale_gate, scale_up, router = pl.pallas_call(
        functools.partial(deliver, experts),
        out_shape=(
            jax.ShapeDtypeStruct((experts, narrow, rows * n), bf16),
            jax.ShapeDtypeStruct((experts, narrow, rows * n), bf16),
            jax.ShapeDtypeStruct((experts, narrow), f32),
            jax.ShapeDtypeStruct((experts, narrow), f32),
            jax.ShapeDtypeStruct((router_rows * nz, rows * n), bf16),
        ),
        in_specs=[vmem] * 4,
        out_specs=(hbm,) * 5,
        scratch_shapes=[dma((2 * experts + 3,))],
        compiler_params=pltpu.CompilerParams(vmem_limit_bytes=1048576),
        name="deliver",
    )(*(pltpu.with_memory_space_constraint(x, pltpu.VMEM) for x in results))
    return (final_gate.swapaxes(1, 2), final_up.swapaxes(1, 2), scale_gate, scale_up, router.T)


def solution(mesh):
    n, nz = mesh.shape["shard"], mesh.shape["expert"]

    def local(master_gate, master_up, router_weight, router_gain):
        experts, rows, width = master_gate.shape
        slabs = 2 * experts
        held = (
            (2 * HELD + STREAM) * rows * width * 4 + SLOTS * rows * width * 2
            + slabs * rows * width * 2 + 16 * slabs * width * 4
        )
        fits = (
            n == 8 and nz > 1 and held <= VMEM_LIMIT - 2 * SPARE
            and rows % LANES == 0 and width % LANES == 0 and width % (16 * n) == 0
            and experts >= HELD + 6 and router_weight.shape[1] % 16 == 0
        )
        if not fits:
            return plain(master_gate, master_up, router_weight, router_gain)
        return fused(n, nz, master_gate, master_up, router_weight, router_gain)

    in_specs = (
        P("expert", "shard", None),
        P("expert", "shard", None),
        P("shard", "expert"),
        P("shard"),
    )
    out_specs = (
        P("expert", None, "shard"),
        P("expert", None, "shard"),
        P("expert", "shard"),
        P("expert", "shard"),
        P(),
    )
    return jax.shard_map(local, mesh=mesh, in_specs=in_specs, out_specs=out_specs, check_vma=False)
```

```python
import functools

import jax
import jax.numpy as jnp
from jax import lax
from jax.experimental import pallas as pl
from jax.experimental.pallas import tpu as pltpu
from jax.sharding import PartitionSpec as P

LANES = 128
HELD = 4
STREAM = 6
SLOTS = 4
DEPTH = 3
PHASES = ((6, 1), (2, 4), (7,), (3, 5))
EARLY = ((2, 4, 6),)
LATE = ((2,), (4,))
VMEM_LIMIT = 67043328
SPARE = 4194304

def plain(master_gate, master_up, router_weight, router_gain):
    total_gate, total_up = lax.psum(
        (jnp.sum(master_gate * master_gate, axis=1), jnp.sum(master_up * master_up, axis=1)),
        "shard",
    )
    scale_gate = jnp.sqrt(total_gate)
    scale_up = jnp.sqrt(total_up)
    narrow_gate, narrow_up = (
        (master_gate / jnp.expand_dims(scale_gate, 1)).astype(jnp.bfloat16),
        (master_up / jnp.expand_dims(scale_up, 1)).astype(jnp.bfloat16),
    )
    final_gate, final_up = (
        lax.all_to_all(narrow_gate, "shard", split_axis=2, concat_axis=1, tiled=True),
        lax.all_to_all(narrow_up, "shard", split_axis=2, concat_axis=1, tiled=True),
    )
    scale_gate = lax.dynamic_slice_in_dim(
        scale_gate, lax.axis_index("shard") * final_gate.shape[2], final_gate.shape[2], axis=1
    )
    scale_up = lax.dynamic_slice_in_dim(
        scale_up, lax.axis_index("shard") * final_up.shape[2], final_up.shape[2], axis=1
    )
    part_router = (router_weight * router_gain[:, None]).astype(jnp.bfloat16)
    row_router = lax.all_gather(part_router, "shard", axis=0, tiled=True)
    serve_router = lax.all_gather(row_router, "expert", axis=1, tiled=True)
    return (final_gate, final_up, scale_gate, scale_up, serve_router)


def partner(me, n, mask):
    index, bit = 0, 1
    while bit < n:
        mine = lax.rem(me // bit, 2)
        index = index + bit * (1 - mine if mask & bit else mine)
        bit *= 2
    return index


def raw_rows_of(narrow, experts):
    return narrow * experts // 61 // 16 * 16


def peers_of(stages):
    return sum(len(stage) for stage in stages)


def remote(source, target, send, recv, device):
    return pltpu.make_async_remote_copy(
        src_ref=source, dst_ref=target, send_sem=send, recv_sem=recv,
        device_id=device, device_id_type=pl.DeviceIdType.MESH)


def kernel(n, nz, gate, up, weight, gain, out, scale_gate, scale_up, router_out,
           buf, stream, slots, part0, got0, part1, got1, run1, total1, part2, got2, run2, total2,
           scales, inverse, weight_in, gain_in, piece, column,
           load_sem, stream_sem, router_sem, send_sem, recv_sem, raw_sem, rest_sem,
           send0, recv0, send1, recv1, send2, recv2,
           first_send, first_recv, second_send, second_recv, third_send, third_recv, go):
    me = lax.axis_index("shard")
    mez = lax.axis_index("expert")
    core = lax.rem(me, 2)
    experts, rows, width = gate.shape
    narrow = width // n
    raw_rows = raw_rows_of(narrow, experts)
    tiles = width // LANES
    router_rows = weight.shape[0]
    sources = (gate, up)
    ring = 2 * HELD

    def load(src, e):
        k = (2 * e + src) % ring
        return pltpu.make_async_copy(sources[src].at[e], buf.at[k], load_sem.at[k])

    def flow(src, e):
        k = (2 * (e - HELD) + src) % STREAM
        return pltpu.make_async_copy(sources[src].at[e], stream.at[k], stream_sem.at[k])

    for e in range(HELD):
        for src in range(2):
            load(src, e).start()
    weight_load = pltpu.make_async_copy(weight, weight_in, router_sem.at[0])
    gain_load = pltpu.make_async_copy(gain, gain_in, router_sem.at[1])
    weight_load.start()
    gain_load.start()
    for e in range(HELD, HELD + STREAM // 2):
        for src in range(2):
            flow(src, e).start()

    barrier = pltpu.get_barrier_semaphore()
    for chip in range(n // 2):
        @pl.when(me != 2 * chip)
        def _():
            pl.semaphore_signal(barrier, inc=1, device_id={"shard": 2 * chip},
                                device_id_type=pl.DeviceIdType.MESH)

    @pl.when(core == 1)
    def _():
        for r in range(1, nz):
            pl.semaphore_signal(barrier, inc=1, device_id={"expert": lax.rem(mez + r, nz)},
                                device_id_type=pl.DeviceIdType.MESH)

    @pl.when(core == 0)
    def _():
        pl.semaphore_wait(barrier, n - 1)
        pl.semaphore_signal(go, inc=1, device_id={"shard": partner(me, n, 1)},
                            device_id_type=pl.DeviceIdType.MESH)

    def greeted():
        @pl.when(core == 1)
        def _():
            pl.semaphore_wait(go, 1)

    my_lanes = pl.ds(pl.multiple_of(me * rows, rows), rows)
    my_rows = pl.ds(pl.multiple_of(me * narrow, 16), narrow)

    def slab_copy(src, e, mask, raw=False):
        s = (2 * e + src) % SLOTS
        target = partner(me, n, mask)
        begin, count = target * narrow, narrow
        first = isinstance(e, int) and e == 0
        sem = recv_sem
        if raw:
            s, count, sem = 2 + src, raw_rows, raw_sem
        elif first:
            sem = rest_sem
            if mask > 1:
                begin, count = begin + raw_rows, narrow - raw_rows
        return remote(
            slots.at[s, pl.ds(pl.multiple_of(begin, 16), count), :],
            out.at[src * experts + e, narrow - count if first and not raw else 0:count if raw else narrow, my_lanes]
            if first else out.at[src * experts + e, :, my_lanes],
            send_sem.at[s, mask - 1], sem.at[src, mask - 1], {"shard": target})

    def raw_slab(src):
        def tile(j, _):
            lanes = pl.ds(pl.multiple_of(j * LANES, LANES), LANES)
            slots[2 + src, lanes, :] = buf[src, :, lanes].T.astype(jnp.bfloat16)
            return 0

        lax.fori_loop(0, tiles, tile, 0, unroll=True)

    def raw_send(src):
        for mask in range(2, n):
            slab_copy(src, 0, mask, True).start()

    def wait_phase(src, e, q):
        if isinstance(e, int) and e < 0:
            raw = len(PHASES) * (2 * e + src) + q + 2
            if raw >= 0:
                for mask in range(2, n):
                    slab_copy(raw, 0, mask, True).wait_send()
            return
        for mask in PHASES[q]:
            slab_copy(src, e, mask).wait_send()

    def phase(src, e, q):
        back, before = q - DEPTH, src
        while back < 0:
            back += len(PHASES)
            before -= 1
        wait_phase(before % 2, e + before // 2, back)
        for mask in PHASES[q]:
            slab_copy(src, e, mask).start()

    def narrow_slab(src, e):
        k = 2 * e + src
        b, s = k % ring, k % SLOTS
        if not isinstance(e, int) or e >= HELD:
            load(src, e).wait()

        def tile(j, _):
            lanes = pl.ds(pl.multiple_of(j * LANES, LANES), LANES)
            y = buf[b, :, lanes] * inverse[src, j, pl.ds(e, 1), :]
            slots[s, lanes, :] = y.T.astype(jnp.bfloat16)
            return 0

        lax.fori_loop(0, tiles, tile, 0, unroll=True)
        out[src * experts + e, :, my_lanes] = slots[s, my_rows, :]
        if isinstance(e, int):
            if e + HELD < experts:
                load(src, e + HELD).start()
        else:
            @pl.when(e + HELD < experts)
            def _():
                load(src, e + HELD).start()

    def squares(x):
        return jnp.sum(x * x, axis=0, keepdims=True)

    def sums_held(src, e):
        load(src, e).wait()
        value = squares(buf[2 * e + src])
        if e == 0:
            part0[src] = value
        else:
            part1[src, e - 1:e, :] = value

    def sums_stream(begin, end):
        def one(e, _):
            for src in range(2):
                flow(src, e).wait()
                part2[src, pl.ds(e - HELD, 1), :] = squares(stream[(2 * (e - HELD) + src) % STREAM])

                @pl.when(e + STREAM // 2 < experts)
                def _():
                    flow(src, e + STREAM // 2).start()
            return 0
        lax.fori_loop(begin, end, one, 0)

    def keep(src, begin, end, total):
        scale = jnp.sqrt(total)
        scales[src, begin:end, :] = scale
        reciprocal = 1.0 / scale
        for j in range(tiles):
            inverse[src, j, begin:end, :] = reciprocal[:, j * LANES:(j + 1) * LANES]

    def greet(mask):
        return remote(part0, got0.at[mask - 1], send0.at[mask - 1], recv0.at[mask - 1],
                      {"shard": partner(me, n, mask)})

    def greet_end():
        for mask in range(1, n):
            greet(mask).wait()
        for src in range(2):
            total = part0[src]
            for mask in range(1, n):
                total = total + got0[mask - 1, src]
            keep(src, 0, 1, total)

    class Sums:
        def __init__(self, stages, begin, end, part, got, run, total, send, recv):
            self.stages, self.begin, self.end = stages, begin, end
            self.part, self.got, self.run, self.total = part, got, run, total
            self.send, self.recv = send, recv

        def copy(self, source, target, i, mask):
            return remote(source, target, self.send.at[i], self.recv.at[i],
                          {"shard": partner(me, n, mask)})

        def swap(self):
            return self.copy(self.part.at[1 - core], self.got.at[0], 0, 1)

        def swap_end(self):
            self.swap().wait()
            self.run[0] = self.part[core] + self.got[0]

        def passes(self, s):
            first = 1 + peers_of(self.stages[:s])
            return [self.copy(self.run.at[s], self.got.at[first + i], first + i, mask)
                    for i, mask in enumerate(self.stages[s])]

        def pass_start(self, s):
            for copy in self.passes(s):
                copy.start()

        def pass_end(self, s):
            value = self.run[s]
            for i, copy in enumerate(self.passes(s)):
                copy.wait()
                value = value + self.got[1 + peers_of(self.stages[:s]) + i]
            if s + 1 < len(self.stages):
                self.run[s + 1] = value
            else:
                self.total[core] = value

        def share(self):
            half = self.total.at[core]
            return self.copy(half, half, 1 + peers_of(self.stages), 1)

        def finish(self):
            self.share().wait()
            for src in range(2):
                keep(src, self.begin, self.end, self.total[src])

    early = Sums(EARLY, 1, HELD, part1, got1, run1, total1, send1, recv1)
    late = Sums(LATE, HELD, experts, part2, got2, run2, total2, send2, recv2)

    def mine(x):
        chosen = x[:, :narrow]
        for t in range(1, n):
            chosen = jnp.where(me == t, x[:, t * narrow:(t + 1) * narrow], chosen)
        return chosen

    def first_copy(mask):
        return remote(piece, column.at[:, my_lanes], first_send.at[mask - 1], first_recv.at[mask - 1],
                      {"shard": partner(me, n, mask)})

    my_columns = pl.ds(pl.multiple_of(mez * router_rows, router_rows), router_rows)

    def second_copy(r):
        return remote(column, router_out.at[my_columns, :], second_send.at[r - 1], second_recv.at[r - 1],
                      {"expert": lax.rem(mez + r, nz)})

    def third_copy(r):
        theirs = pl.ds(pl.multiple_of(lax.rem(mez + r, nz) * router_rows, router_rows), router_rows)
        return remote(router_out.at[theirs, :], router_out.at[theirs, :],
                      third_send.at[r - 1], third_recv.at[r - 1], {"shard": partner(me, n, 1)})

    def settle(src):
        row = 1.0 / mine(scales[src, 0:1, :])
        pad = -narrow % LANES
        if pad:
            row = jnp.concatenate([row, jnp.zeros((1, pad), jnp.float32)], axis=1)
        factor = jnp.broadcast_to(row, (LANES, narrow + pad)).T[:raw_rows]
        for mask in range(2, n):
            slab_copy(src, 0, mask, True).wait_recv()
            begin = partner(me, n, mask) * rows
            for j in range(rows // LANES):
                lanes = pl.ds(pl.multiple_of(begin + j * LANES, LANES), LANES)
                y = out[src * experts, :raw_rows, lanes].astype(jnp.float32) * factor
                out[src * experts, :raw_rows, lanes] = y.astype(jnp.bfloat16)

    last = len(PHASES)
    half = last // 2
    steps = experts - HELD
    cuts = [HELD + steps * i // 6 for i in range(7)]

    def chunk(i):
        sums_stream(cuts[i], cuts[i + 1])

    def run(k, begin, end):
        for q in range(begin, end):
            phase(k % 2, k // 2, q)

    def ahead(k):
        narrow_slab(k % 2, k // 2)

    sums_held(0, 0)
    sums_held(1, 0)
    raw_slab(0)
    greeted()
    for mask in range(1, n):
        greet(mask).start()
    raw_send(0)
    raw_slab(1)
    raw_send(1)
    for e in range(1, HELD):
        for src in range(2):
            sums_held(src, e)
    early.swap().start()
    greet_end()
    ahead(0)
    run(0, 0, 1)
    early.swap_end()
    early.pass_start(0)
    run(0, 1, 4)
    ahead(1)
    run(1, 0, 2)
    weight_load.wait()
    gain_load.wait()
    value = (weight_in[...] * gain_in[...]).astype(jnp.bfloat16)
    piece[...] = value
    column[:, my_lanes] = value
    for mask in range(1, n):
        first_copy(mask).start()
    chunk(0)
    run(1, 2, 3)
    chunk(1)
    early.pass_end(0)
    early.share().start()
    run(1, 3, 4)
    early.finish()
    ahead(2)
    run(2, 0, 1)
    chunk(2)
    chunk(3)
    run(2, 1, 2)
    ahead(3)
    run(2, 2, 3)
    chunk(4)
    run(2, 3, 4)
    chunk(5)
    late.swap().start()
    run(3, 0, 1)
    late.swap_end()
    late.pass_start(0)
    run(3, 1, half)
    ahead(4)
    run(3, half, last)
    run(4, 0, half)
    late.pass_end(0)
    late.pass_start(1)
    ahead(5)
    run(4, half, last)
    run(5, 0, half)
    late.pass_end(1)
    late.share().start()
    ahead(6)
    run(5, half, last)
    late.finish()
    run(6, 0, half)
    ahead(7)
    for src in range(2):
        settle(src)
    run(6, half, last)
    for mask in range(1, n):
        first_copy(mask).wait()
    router_out[my_columns, :] = column[...]

    @pl.when(core == 1)
    def _():
        pl.semaphore_wait(barrier, nz - 1)
        for r in range(1, nz):
            second_copy(r).start()

    run(7, 0, half)
    ahead(8)
    run(7, half, last)

    @pl.when(core == 1)
    def _():
        for r in range(1, nz):
            second_copy(r).wait()
        for r in range(1, nz):
            third_copy(r).start()

    run(8, 0, half)
    ahead(9)
    run(8, half, last)
    run(9, 0, half)
    ahead(10)
    run(9, half, last)

    @pl.when(core == 1)
    def _():
        for r in range(1, nz):
            third_copy(r).wait_send()

    def step(e, _):
        for src in range(2):
            for q in range(half):
                phase(src, e, q)
            if src == 0:
                narrow_slab(1, e)
            else:
                @pl.when(e + 1 < experts)
                def _():
                    narrow_slab(0, e + 1)
            for q in range(half, last):
                phase(src, e, q)
        return 0

    lax.fori_loop(HELD + 1, experts, step, 0)

    for ref, src in ((scale_gate, 0), (scale_up, 1)):
        ref[...] = mine(scales[src])

    @pl.when(core == 0)
    def _():
        for r in range(1, nz):
            third_copy(r).wait_recv()

    for q in range(2 * last - DEPTH, 2 * last):
        wait_phase(q // last, experts - 1, q % last)
    for mask in range(1, n):
        for src in range(2):
            slab_copy(src, 0, mask).wait_recv()
            whole = out.at[src * experts + 1:(src + 1) * experts, :, my_lanes]
            remote(whole, whole, send_sem.at[0, mask - 1], recv_sem.at[src, mask - 1],
                   {"shard": partner(me, n, mask)}).wait_recv()


def deliver(experts, out, scale_gate, scale_up, router,
            to_gate, to_up, to_scale_gate, to_scale_up, to_router, sem):
    pairs = [(scale_gate, to_scale_gate), (scale_up, to_scale_up), (router, to_router)]
    for e in range(experts):
        pairs += [(out.at[e], to_gate.at[e]), (out.at[experts + e], to_up.at[e])]
    copies = [pltpu.make_async_copy(a, b, sem.at[i]) for i, (a, b) in enumerate(pairs)]
    for copy in copies:
        copy.start()
    for copy in copies:
        copy.wait()


def fused(n, nz, master_gate, master_up, router_weight, router_gain):
    experts, rows, width = master_gate.shape
    slabs = 2 * experts
    narrow = width // n
    router_rows = router_weight.shape[1]
    vmem = pl.BlockSpec(memory_space=pltpu.VMEM)
    hbm = pl.BlockSpec(memory_space=pltpu.HBM)
    dma = pltpu.SemaphoreType.DMA
    f32, bf16 = jnp.float32, jnp.bfloat16

    def sums(count, stages):
        peers = peers_of(stages)
        return [
            pltpu.VMEM((2, count, width), f32),
            pltpu.VMEM((1 + peers, count, width), f32),
            pltpu.VMEM((len(stages), count, width), f32),
            pltpu.VMEM((2, count, width), f32),
        ]

    results = pl.pallas_call(
        functools.partial(kernel, n, nz),
        out_shape=(
            pltpu.VMEM((slabs, narrow, rows * n), bf16),
            pltpu.VMEM((experts, narrow), f32),
            pltpu.VMEM((experts, narrow), f32),
            pltpu.VMEM((router_rows * nz, rows * n), bf16),
        ),
        in_specs=[hbm] * 4,
        out_specs=(vmem,) * 4,
        scratch_shapes=[
            pltpu.VMEM((2 * HELD, rows, width), f32),
            pltpu.VMEM((STREAM, rows, width), f32),
            pltpu.VMEM((SLOTS, width, rows), bf16),
            pltpu.VMEM((2, 1, width), f32),
            pltpu.VMEM((n - 1, 2, 1, width), f32),
            *sums(HELD - 1, EARLY),
            *sums(experts - HELD, LATE),
            pltpu.VMEM((2, experts, width), f32),
            pltpu.VMEM((2, width // LANES, experts, LANES), f32),
            pltpu.VMEM((router_rows, rows), f32),
            pltpu.VMEM((1, rows), f32),
            pltpu.VMEM((router_rows, rows), bf16),
            pltpu.VMEM((router_rows, rows * n), bf16),
            dma((2 * HELD,)), dma((STREAM,)), dma((2,)),
            dma((SLOTS, n - 1)), dma((2, n - 1)), dma((2, n - 1)), dma((2, n - 1)),
            dma((n - 1,)), dma((n - 1,)),
            dma((2 + peers_of(EARLY),)), dma((2 + peers_of(EARLY),)),
            dma((2 + peers_of(LATE),)), dma((2 + peers_of(LATE),)),
            dma((n - 1,)), dma((n - 1,)), dma((nz - 1,)), dma((nz - 1,)),
            dma((nz - 1,)), dma((nz - 1,)), pltpu.SemaphoreType.REGULAR,
        ],
        compiler_params=pltpu.CompilerParams(
            collective_id=0, has_side_effects=True,
            vmem_limit_bytes=VMEM_LIMIT - slabs * narrow * rows * n * 2 - SPARE),
        name="exchange",
    )(master_gate, master_up, router_weight.T, router_gain[None, :])
    final_gate, final_up, scale_gate, scale_up, router = pl.pallas_call(
        functools.partial(deliver, experts),
        out_shape=(
            jax.ShapeDtypeStruct((experts, narrow, rows * n), bf16),
            jax.ShapeDtypeStruct((experts, narrow, rows * n), bf16),
            jax.ShapeDtypeStruct((experts, narrow), f32),
            jax.ShapeDtypeStruct((experts, narrow), f32),
            jax.ShapeDtypeStruct((router_rows * nz, rows * n), bf16),
        ),
        in_specs=[vmem] * 4,
        out_specs=(hbm,) * 5,
        scratch_shapes=[dma((2 * experts + 3,))],
        compiler_params=pltpu.CompilerParams(vmem_limit_bytes=1048576),
        name="deliver",
    )(*(pltpu.with_memory_space_constraint(x, pltpu.VMEM) for x in results))
    return (final_gate.swapaxes(1, 2), final_up.swapaxes(1, 2), scale_gate, scale_up, router.T)


def solution(mesh):
    n, nz = mesh.shape["shard"], mesh.shape["expert"]

    def local(master_gate, master_up, router_weight, router_gain):
        experts, rows, width = master_gate.shape
        slabs = 2 * experts
        held = (
            (2 * HELD + STREAM) * rows * width * 4 + SLOTS * rows * width * 2
            + slabs * rows * width * 2 + 16 * slabs * width * 4
        )
        fits = (
            n == 8 and nz > 1 and held <= VMEM_LIMIT - 2 * SPARE
            and rows % LANES == 0 and width % LANES == 0 and width % (16 * n) == 0
            and experts >= HELD + 6 and raw_rows_of(width // n, experts) > 0 and router_weight.shape[1] % 16 == 0
        )
        if not fits:
            return plain(master_gate, master_up, router_weight, router_gain)
        return fused(n, nz, master_gate, master_up, router_weight, router_gain)

    in_specs = (
        P("expert", "shard", None),
        P("expert", "shard", None),
        P("shard", "expert"),
        P("shard"),
    )
    out_specs = (
        P("expert", None, "shard"),
        P("expert", None, "shard"),
        P("expert", "shard"),
        P("expert", "shard"),
        P(),
    )
    return jax.shard_map(local, mesh=mesh, in_specs=in_specs, out_specs=out_specs, check_vma=False)
```
